32 devices in a mesh: band: 8 (over z, core), lane: 4 (over y, x).
Axes of the slice: x: 2, y: 2, z: 4, core: 2. Of those that a mesh axis runs over, the one named last changes fastest.
Arguments:
- first_factor: bfloat16 [8192, 4096], P('band', 'lane'), may hold values from -6 to 6
- second_factor: bfloat16 [4096, 2048], P('band', 'lane'), may hold values from -0.09375 to 0.09375
- result_in: float32 [8192, 2048], P('band', 'lane'), may hold values from -6 to 6
- pivot_scale: float32 [4096], replicated, may hold values from 0.25 to 1.75
Outputs:
- updated: float32 [8192, 2048], P('band', 'lane')
The draws below stay inside these ranges and needn't reach their ends.
All inputs are finite; a program needn't handle non-finite values.
Results may differ from the reference program's by a relative error of at most 0.002.
Values may be sent and summed in bfloat16 or wider, within the bound.
No kernel may reach another device: no remote copies, remote signals or barrier semaphores. Data moves between devices by JAX's collectives and lax.ppermute only.
A program may use at most 128 MiB of HBM per device.

```python
import jax
import jax.numpy as jnp
from jax import lax

ROWS = 8192
COLS = 2048
INNER = 4096


def level_of(own_key, shape, split, least, top_value):
    factor_of = 1.0
    for axis_at, parts in split:
        steps = jax.random.uniform(jax.random.fold_in(jax.random.fold_in(own_key, 6), axis_at), (parts,), jnp.float32, least / len(split), top_value / len(split))
        factor_of = factor_of * jnp.repeat(jnp.exp(steps), shape[axis_at] // parts).reshape((-1,) + (1,) * (len(shape) - 1 - axis_at))
    return factor_of


def centred(own_key, shape, deviation, bound, split=(), held_as=jnp.bfloat16):
    result = jax.random.normal(own_key, shape, jnp.float32) * deviation
    if len(split) > 0:
        result = level_of(own_key, shape, split, -0.22, 0.18) * result
    return jnp.clip(result, min=-bound, max=bound).astype(held_as)


def setup_inputs(seed: int = 0) -> dict:
    key_list = jax.random.split(jax.random.key(seed), 5)
    first_factor = centred(key_list[0], (ROWS, INNER), 1.0, 6.0, ((0, 8), (1, 4)))
    second_factor = centred(key_list[1], (INNER, COLS), INNER ** -0.5, 0.09375, ((0, 8), (1, 4)))
    result_in = centred(key_list[2], (ROWS, COLS), 1.0, 6.0, ((0, 8), (1, 4)), jnp.float32)
    pivot_scale = jnp.clip(1.0 + 0.15 * jax.random.normal(key_list[3], (INNER,), jnp.float32), 0.25, 1.75)
    return {"first_factor": first_factor, "second_factor": second_factor, "result_in": result_in, "pivot_scale": pivot_scale}


def reference(first_factor, second_factor, result_in, pivot_scale):
    scaled_left = (first_factor.astype(jnp.float32) * pivot_scale).astype(jnp.bfloat16)
    updated = result_in - jnp.dot(scaled_left, second_factor, preferred_element_type=jnp.float32)
    row_power = lax.optimization_barrier(jnp.sum(updated * updated, axis=1))
    updated = updated * lax.rsqrt(row_power / COLS + 1e-06)[:, None]
    return updated
```

```python
import functools

import jax
import jax.numpy as jnp
from jax import lax
from jax.experimental import pallas as pl
from jax.experimental.pallas import tpu as pltpu
from jax.sharding import PartitionSpec as P


CORES = 2
EPS = 1e-06
LANES = 128
VMEM_LIMIT = 60 * 1024 * 1024


def cost(flops, nbytes):
    return pl.CostEstimate(flops=int(flops), bytes_accessed=int(nbytes), transcendentals=0)


def vmem():
    return pl.BlockSpec(memory_space=pltpu.VMEM)


def params():
    return pltpu.CompilerParams(vmem_limit_bytes=VMEM_LIMIT)


def scale_kernel(lane_ref, left_ref, scale_ref, *outs):
    scale = scale_ref[...].reshape(1, -1)
    height = outs[0].shape[0]
    for at, out in enumerate(outs):
        rows = left_ref[at * height:(at + 1) * height, :]
        out[...] = (rows.astype(jnp.float32) * scale).astype(jnp.bfloat16)


def scaled_pieces(lane, left, scale, block, blocks, count):
    rows, depth = left.shape
    height = rows // blocks
    piece = jax.ShapeDtypeStruct((height // count, depth), jnp.bfloat16)
    return pl.pallas_call(
        scale_kernel,
        grid_spec=pltpu.PrefetchScalarGridSpec(
            num_scalar_prefetch=1,
            grid=(1,),
            in_specs=[
                pl.BlockSpec((height, depth), lambda i, lane: (block, 0)),
                pl.BlockSpec((depth,), lambda i, lane: (lane[0],)),
            ],
            out_specs=[pl.BlockSpec(piece.shape, lambda i, lane: (0, 0))] * count,
        ),
        out_shape=[piece] * count,
        cost_estimate=cost(2 * height * depth, 4 * height * depth),
        compiler_params=params(),
    )(lane, left, scale)


def lay_kernel(chips, where_ref, *refs):
    mine, other, out, sems = refs[:chips], refs[chips:2 * chips], refs[-2], refs[-1]
    depth = mine[0].shape[0]
    z, core = where_ref[0], where_ref[1]
    copies = []
    for step in range(chips):
        base = lax.rem(z - step + chips, chips) * (CORES * depth)
        for at, (source, half) in enumerate(((mine[step], core), (other[step], 1 - core))):
            start = pl.multiple_of(base + half * depth, depth)
            copies.append(
                pltpu.make_async_copy(source, out.at[pl.ds(start, depth), :], sems.at[step, at])
            )
    for copy in copies:
        copy.start()
    for copy in copies:
        copy.wait()


def laid(where, mine, other):
    chips = len(mine)
    depth, width = mine[0].shape
    total = chips * CORES * depth
    return pl.pallas_call(
        functools.partial(lay_kernel, chips),
        in_specs=[pl.BlockSpec(memory_space=pltpu.SMEM)]
        + [pl.BlockSpec(memory_space=pl.ANY)] * (2 * chips),
        out_specs=vmem(),
        out_shape=jax.ShapeDtypeStruct((total, width), jnp.bfloat16),
        scratch_shapes=[pltpu.SemaphoreType.DMA((chips, CORES))],
        cost_estimate=cost(total * width, 4 * total * width),
        compiler_params=params(),
    )(where, *mine, *other)


def product_kernel(plan, squares, where_ref, right_ref, *refs):
    n_rows = len(plan)
    n_left = 1 + max(at for terms in plan for at, _ in terms)
    bases, lefts = refs[:n_rows], refs[n_rows:n_rows + n_left]
    outs = refs[n_rows + n_left + squares:n_rows + n_left + squares + n_rows]
    lane = where_ref[2]
    depth = lefts[0].shape[1]
    for at, terms in enumerate(plan):
        total = bases[at][...]
        for left, distance in terms:
            part = lax.bitwise_xor(lane, distance)
            start = pl.multiple_of(part * depth, depth)
            total = total - jnp.dot(
                lefts[left][...], right_ref[pl.ds(start, depth), :],
                preferred_element_type=jnp.float32,
            )
        outs[at][...] = total


def power_rows(block):
    squares = block * block
    folded = squares[:, :LANES]
    for at in range(1, block.shape[1] // LANES):
        folded = folded + squares[:, at * LANES:(at + 1) * LANES]
    return jnp.sum(folded.T, axis=0, keepdims=True)


def products(where, right, bases, lefts, plan):
    flops = sum(2 * lefts[at].shape[0] * lefts[at].shape[1] * right.shape[1] for terms in plan for at, _ in terms)
    return pl.pallas_call(
        functools.partial(product_kernel, plan, 0),
        in_specs=[pl.BlockSpec(memory_space=pltpu.SMEM)] + [vmem()] * (1 + len(bases) + len(lefts)),
        out_specs=[vmem()] * len(bases),
        out_shape=[jax.ShapeDtypeStruct(base.shape, jnp.float32) for base in bases],
        cost_estimate=cost(flops, flops / 512),
        compiler_params=params(),
    )(where, right, *bases, *lefts)


def first_kernel(plan, where_ref, right_ref, base_ref, *refs):
    height = refs[0].shape[0]
    bases = [base_ref.at[at * height:(at + 1) * height, :] for at in range(len(plan))]
    product_kernel(plan, 0, where_ref, right_ref, *bases, *refs)


def first_products(where, right, base, lefts, plan):
    height = lefts[0].shape[0]
    flops = sum(2 * height * lefts[at].shape[1] * right.shape[1] for terms in plan for at, _ in terms)
    return pl.pallas_call(
        functools.partial(first_kernel, plan),
        in_specs=[pl.BlockSpec(memory_space=pltpu.SMEM)] + [vmem()] * (2 + len(lefts)),
        out_specs=[vmem()] * len(plan),
        out_shape=[jax.ShapeDtypeStruct((height, base.shape[1]), jnp.float32)] * len(plan),
        cost_estimate=cost(flops, flops / 512),
        compiler_params=params(),
    )(where, right, base, *lefts)


def last_kernel(plan, n_done, where_ref, right_ref, *refs):
    n_rows = len(plan)
    n_left = 1 + max(at for terms in plan for at, _ in terms)
    done, rest = refs[:n_done], refs[n_done:]
    power_ref = rest[-1]
    product_kernel(plan, 0, where_ref, right_ref, *rest[:-1])
    outs = rest[n_rows + n_left:-1]
    at = 0
    for ref in (*done, *outs):
        for block in range(ref.shape[0] // LANES):
            power_ref[at:at + 1, :] = power_rows(ref[block * LANES:(block + 1) * LANES, :])
            at += 1


def last_products(where, right, done, bases, lefts, plan):
    flops = sum(2 * lefts[at].shape[0] * lefts[at].shape[1] * right.shape[1] for terms in plan for at, _ in terms)
    rows = sum(a.shape[0] for a in (*done, *bases))
    *outs, power = pl.pallas_call(
        functools.partial(last_kernel, plan, len(done)),
        in_specs=[pl.BlockSpec(memory_space=pltpu.SMEM)]
        + [vmem()] * (1 + len(done) + len(bases) + len(lefts)),
        out_specs=[vmem()] * (len(bases) + 1),
        out_shape=[jax.ShapeDtypeStruct(base.shape, jnp.float32) for base in bases]
        + [jax.ShapeDtypeStruct((rows // LANES, LANES), jnp.float32)],
        cost_estimate=cost(flops, flops / 512),
        compiler_params=params(),
    )(where, right, *done, *bases, *lefts)
    return outs, power


def norm_kernel(columns, n_power, *refs):
    powers, blocks, out = refs[:n_power], refs[n_power:-1], refs[-1]
    power = powers[0][...]
    for ref in powers[1:]:
        power = power + ref[...]
    factor = lax.rsqrt(power / columns + EPS)
    at = 0
    for ref in blocks:
        for block in range(ref.shape[0] // LANES):
            spread = jnp.broadcast_to(factor[at:at + 1, :], (LANES, LANES)).T
            for tile in range(ref.shape[1] // LANES):
                columns_at = slice(tile * LANES, (tile + 1) * LANES)
                out[at * LANES:(at + 1) * LANES, columns_at] = (
                    ref[block * LANES:(block + 1) * LANES, columns_at] * spread
                )
            at += 1


def normed(columns, powers, blocks):
    rows = sum(block.shape[0] for block in blocks)
    width = blocks[0].shape[1]
    return pl.pallas_call(
        functools.partial(norm_kernel, columns, len(powers)),
        in_specs=[vmem()] * (len(powers) + len(blocks)),
        out_specs=vmem(),
        out_shape=jax.ShapeDtypeStruct((rows, width), jnp.float32),
        cost_estimate=cost(rows * width, 8 * rows * width),
        compiler_params=params(),
    )(*powers, *blocks)


def square_lanes(first_factor, second_factor, result_in, pivot_scale):
    return square_lanes_body(first_factor, second_factor, result_in, pivot_scale)


def square_lanes_body(first_factor, second_factor, result_in, pivot_scale):
    bands, lanes = lax.axis_size("band"), lax.axis_size("lane")
    chips = bands // CORES
    band, lane = lax.axis_index("band"), lax.axis_index("lane")
    where = jnp.stack([band // CORES, band % CORES, lane]).astype(jnp.int32)

    def send(axis, perm, value):
        return lax.ppermute(value, axis, perm)

    def across(distance):
        return [(l, l ^ distance) for l in range(lanes)]

    def px(value):
        return send("lane", across(1), value)

    def py(value):
        return send("lane", across(2), value)

    def pd(value):
        return send("lane", across(3), value)

    up = [(b, (b + CORES) % bands) for b in range(bands)]
    swap = [(b, b ^ 1) for b in range(bands)]

    lane_at = where[2:]
    own_t0, own_b0 = scaled_pieces(lane_at, first_factor, pivot_scale, 0, 2, 2)
    own_t1, own_b1 = scaled_pieces(lane_at, first_factor, pivot_scale, 1, 2, 2)

    mine = [second_factor]
    for _ in range(1, chips):
        mine.append(send("band", up, mine[-1]))
    other = [send("band", swap, piece) for piece in mine]

    x_t0, y_b0 = px(own_t0), py(own_b0)
    x_b0, y_t0 = px(own_b0), py(own_t0)
    x_t1, y_b1 = px(own_t1), py(own_b1)
    d_b0, d_t0 = px(y_b0), py(x_t0)
    x_b1, y_t1 = px(own_b1), py(own_t1)
    d_b1, d_t1 = px(y_b1), py(x_t1)

    right = laid(where, mine, other)
    lefts = [own_t0, own_b0, own_t1, own_b1, x_t0, x_b0, x_t1, y_t0, y_b0, y_b1]
    plan = [
        [(0, 0), (4, 1), (7, 2)],
        [(1, 0), (5, 1), (8, 2)],
        [(2, 0), (6, 1)],
        [(3, 0), (9, 2)],
    ]
    t0, b0, t1, b1 = first_products(where, right, result_in, lefts, plan)
    t0, b0, t1, b1 = products(
        where, right, [t0, b0, t1, b1], [d_t0, d_b0, y_t1, x_b1],
        [[(0, 3)], [(1, 3)], [(2, 2)], [(3, 1)]],
    )
    (t1, b1), power = last_products(
        where, right, [t0, b0], [t1, b1], [d_t1, d_b1], [[(0, 3)], [(1, 3)]]
    )
    columns = result_in.shape[1] * lanes
    powers = [power, px(power), py(power), pd(power)]
    return normed(columns, powers, [t0, b0, t1, b1])


def any_lanes(first_factor, second_factor, result_in, pivot_scale):
    share = first_factor.shape[1]
    part_scale = lax.dynamic_slice_in_dim(pivot_scale, lax.axis_index("lane") * share, share)
    scaled_left = (first_factor.astype(jnp.float32) * part_scale).astype(jnp.bfloat16)
    left_line = lax.all_gather(scaled_left, "lane", axis=1, tiled=True)
    right_line = lax.all_gather(second_factor, "band", axis=0, tiled=True)
    total = jnp.dot(left_line, right_line, preferred_element_type=jnp.float32)
    updated = result_in - total
    row_power = lax.psum(jnp.sum(updated * updated, axis=1), "lane")
    columns = updated.shape[1] * lax.axis_size("lane")
    return updated * lax.rsqrt(row_power / columns + EPS)[:, None]


def solution(mesh):
    square = mesh.shape["lane"] == 4 and mesh.shape["band"] == 4 * CORES
    return jax.shard_map(
        square_lanes if square else any_lanes,
        mesh=mesh,
        in_specs=(P("band", "lane"), P("band", "lane"), P("band", "lane"), P()),
        out_specs=P("band", "lane"),
        check_vma=False,
    )
```

```python
import functools

import jax
import jax.numpy as jnp
from jax import lax
from jax.experimental import pallas as pl
from jax.experimental.pallas import tpu as pltpu
from jax.sharding import PartitionSpec as P


CORES = 2
EPS = 1e-06
LANES = 128
MIB = 1024 * 1024


def cost(flops, nbytes):
    return pl.CostEstimate(flops=int(flops), bytes_accessed=int(nbytes), transcendentals=0)


def vmem():
    return pl.BlockSpec(memory_space=pltpu.VMEM)


def params(mib):
    return pltpu.CompilerParams(vmem_limit_bytes=mib * MIB)


def smem():
    return pl.BlockSpec(memory_space=pltpu.SMEM)


def scale_kernel(lane_ref, left_ref, scale_ref, *outs):
    scale = scale_ref[...].reshape(1, -1)
    height = outs[0].shape[0]
    for at, out in enumerate(outs):
        rows = left_ref[at * height:(at + 1) * height, :]
        out[...] = (rows.astype(jnp.float32) * scale).astype(jnp.bfloat16)


def scaled_pieces(lane, left, scale, block, blocks, count):
    rows, depth = left.shape
    height = rows // blocks
    piece = jax.ShapeDtypeStruct((height // count, depth), jnp.bfloat16)
    return pl.pallas_call(
        scale_kernel,
        grid_spec=pltpu.PrefetchScalarGridSpec(
            num_scalar_prefetch=1,
            grid=(1,),
            in_specs=[
                pl.BlockSpec((height, depth), lambda i, lane: (block, 0)),
                pl.BlockSpec((depth,), lambda i, lane: (lane[0],)),
            ],
            out_specs=[pl.BlockSpec(piece.shape, lambda i, lane: (0, 0))] * count,
        ),
        out_shape=[piece] * count,
        cost_estimate=cost(2 * height * depth, 4 * height * depth),
        compiler_params=params(60),
    )(lane, left, scale)


def bring(where_ref, first, agreeing, others, out, sems):
    z, core, lane, agree = where_ref[0], where_ref[1], where_ref[2], where_ref[3]

    def both(pieces):
        copies = []
        for at, (distance, mine, other) in enumerate(pieces):
            depth = mine.shape[0]
            ahead = lax.bitwise_xor(z, distance) == lax.bitwise_xor(lane, first)
            slot = jnp.where(ahead, 0, CORES * depth)
            for part, (source, half) in enumerate(((mine, core), (other, 1 - core))):
                start = pl.multiple_of(slot + half * depth, depth)
                copies.append(
                    pltpu.make_async_copy(source, out.at[pl.ds(start, depth), :], sems.at[at, part])
                )
        for copy in copies:
            copy.start()
        for copy in copies:
            copy.wait()

    @pl.when(agree == 1)
    def _():
        both(agreeing)

    @pl.when(agree == 0)
    def _():
        both(others)


def split(pieces):
    distances = [distance for distance, _ in pieces]
    arrays = [array for _, pair in pieces for array in pair]

    def joined_again(refs):
        rows = [(distances[at], *refs[2 * at:2 * at + 2]) for at in range(4)]
        return rows[:2], rows[2:]

    return arrays, joined_again


def block_of(pieces):
    depth, width = pieces[0][1][0].shape
    return jax.ShapeDtypeStruct((2 * CORES * depth, width), jnp.bfloat16)


def bring_one(where_ref, agreeing, others, out, sems):
    core, agree = where_ref[1], where_ref[3]

    def one(pair):
        copies = []
        for part, (source, half) in enumerate(((pair[0], core), (pair[1], 1 - core))):
            depth = source.shape[0]
            start = pl.multiple_of(half * depth, depth)
            copies.append(
                pltpu.make_async_copy(source, out.at[pl.ds(start, depth), :], sems.at[part])
            )
        for copy in copies:
            copy.start()
        for copy in copies:
            copy.wait()

    @pl.when(agree == 1)
    def _():
        one(agreeing)

    @pl.when(agree == 0)
    def _():
        one(others)


def is_own(where_ref, distances):
    z, lane, agree = where_ref[0], where_ref[2], where_ref[3]
    distance = jnp.where(agree == 1, distances[0], distances[1])
    return lax.bitwise_xor(z, distance) == lane


def dot(left, right):
    return jnp.dot(left, right, preferred_element_type=jnp.float32)


def partial_first(where, pieces, own, side):
    arrays, again = split(pieces)
    block = block_of(pieces)
    rows, deep = own.shape
    width = block.shape[1]

    def kernel(where_ref, *refs):
        own_ref, side_ref, sent_ref, right_ref, sems = refs[8:]
        bring(where_ref, 0, *again(refs[:8]), right_ref, sems)
        total = dot(own_ref[...], right_ref[:deep, :]) + dot(side_ref[...], right_ref[deep:, :])
        sent_ref[...] = total.astype(jnp.bfloat16)

    return pl.pallas_call(
        kernel,
        in_specs=[smem()] + [pl.BlockSpec(memory_space=pl.ANY)] * 8 + [vmem()] * 2,
        out_specs=[vmem()] * 2,
        out_shape=[jax.ShapeDtypeStruct((rows, width), jnp.bfloat16), block],
        scratch_shapes=[pltpu.SemaphoreType.DMA((2, CORES))],
        cost_estimate=cost(4 * rows * deep * width, 4 * deep * width),
        compiler_params=params(16),
    )(where, *arrays, own, side)


def partial_kernel(count, right_ref, *refs):
    owns, sides, outs = refs[:count], refs[count:2 * count], refs[2 * count:]
    deep = owns[0].shape[1]
    for own, side, out in zip(owns, sides, outs):
        total = dot(own[...], right_ref[:deep, :]) + dot(side[...], right_ref[deep:, :])
        out[...] = total.astype(jnp.bfloat16)


def partials(right, owns, sides):
    count = len(owns)
    rows, deep = owns[0].shape
    width = right.shape[1]
    return pl.pallas_call(
        functools.partial(partial_kernel, count),
        in_specs=[vmem()] * (1 + 2 * count),
        out_specs=[vmem()] * count,
        out_shape=[jax.ShapeDtypeStruct((rows, width), jnp.bfloat16)] * count,
        cost_estimate=cost(4 * count * rows * deep * width, 4 * deep * width),
        compiler_params=params(20),
    )(right, *owns, *sides)


def kept(where, distances, pieces, base, owns, sides):
    count = len(owns)
    height, deep = owns[0].shape
    width = base.shape[1]

    def kernel(where_ref, *refs):
        base_ref, lefts = refs[4], refs[5:5 + 2 * count]
        outs, right_ref, sems = refs[5 + 2 * count:5 + 3 * count], refs[-2], refs[-1]
        bring_one(where_ref, refs[:2], refs[2:4], right_ref, sems)
        own = is_own(where_ref, distances)

        def products(chosen):
            for at in range(count):
                outs[at][...] = base_ref[at * height:(at + 1) * height, :] - dot(
                    chosen[at][...], right_ref[...]
                )

        pl.when(own)(lambda: products(lefts[:count]))
        pl.when(jnp.logical_not(own))(lambda: products(lefts[count:]))

    flops = 2 * count * height * deep * width
    return pl.pallas_call(
        kernel,
        in_specs=[smem()] + [pl.BlockSpec(memory_space=pl.ANY)] * 4 + [vmem()] * (1 + 2 * count),
        out_specs=[vmem()] * count,
        out_shape=[jax.ShapeDtypeStruct((height, width), jnp.float32)] * count,
        scratch_shapes=[
            pltpu.VMEM((deep, width), jnp.bfloat16), pltpu.SemaphoreType.DMA((CORES,))
        ],
        cost_estimate=cost(flops, flops / 512),
        compiler_params=params(24),
    )(where, *pieces[0], *pieces[1], base, *owns, *sides)


def power_rows(block):
    squares = block * block
    folded = squares[:, :LANES]
    for at in range(1, block.shape[1] // LANES):
        folded = folded + squares[:, at * LANES:(at + 1) * LANES]
    return jnp.sum(folded.T, axis=0, keepdims=True)


def put_powers(ref, power_ref, at):
    for block in range(ref.shape[0] // LANES):
        power_ref[at:at + 1, :] = power_rows(ref[block * LANES:(block + 1) * LANES, :])
        at += 1
    return at


def joined(where, distances, pieces, keeps, gots, owns, sides, before):
    count = len(keeps)
    height, deep = owns[0].shape
    width = keeps[0].shape[1]
    block = jax.ShapeDtypeStruct((deep, width), jnp.bfloat16)
    done = before[1].shape[0] if before else 0
    n_first = 2 if before else 4

    def kernel(where_ref, *refs):
        first, rest = refs[:n_first], refs[n_first:]
        kept_refs, got_refs, lefts = rest[:count], rest[count:2 * count], rest[2 * count:4 * count]
        outs, power_ref = rest[4 * count:5 * count], rest[5 * count]
        if before:
            right_ref = first[0]
            power_ref[:done, :] = first[1][...]
        else:
            right_ref = rest[5 * count + 1]
            bring_one(where_ref, first[:2], first[2:], right_ref, rest[5 * count + 2])
        own = is_own(where_ref, distances)

        def products(chosen):
            for at in range(count):
                total = dot(chosen[at][...], right_ref[...])
                outs[at][...] = kept_refs[at][...] - total - got_refs[at][...].astype(jnp.float32)

        pl.when(own)(lambda: products(lefts[:count]))
        pl.when(jnp.logical_not(own))(lambda: products(lefts[count:]))
        at = done
        for out in outs:
            at = put_powers(out, power_ref, at)

    flops = 2 * count * height * deep * width
    results = pl.pallas_call(
        kernel,
        in_specs=[smem()]
        + [vmem() if before else pl.BlockSpec(memory_space=pl.ANY)] * n_first
        + [vmem()] * (4 * count),
        out_specs=[vmem()] * (count + 1 + (not before)),
        out_shape=[jax.ShapeDtypeStruct((height, width), jnp.float32)] * count
        + [jax.ShapeDtypeStruct((done + count * height // LANES, LANES), jnp.float32)]
        + ([] if before else [block]),
        scratch_shapes=[] if before else [pltpu.SemaphoreType.DMA((CORES,))],
        cost_estimate=cost(flops, flops / 256),
        compiler_params=params(16),
    )(where, *(before if before else (*pieces[0], *pieces[1])), *keeps, *gots, *owns, *sides)
    return results[:count], results[count], None if before else results[count + 1]


def norm_kernel(columns, n_power, *refs):
    powers, blocks, out = refs[:n_power], refs[n_power:-1], refs[-1]
    power = powers[0][...]
    for ref in powers[1:]:
        power = power + ref[...]
    factor = lax.rsqrt(power / columns + EPS)
    at = 0
    for ref in blocks:
        for block in range(ref.shape[0] // LANES):
            spread = jnp.broadcast_to(factor[at:at + 1, :], (LANES, LANES)).T
            for tile in range(ref.shape[1] // LANES):
                columns_at = slice(tile * LANES, (tile + 1) * LANES)
                out[at * LANES:(at + 1) * LANES, columns_at] = (
                    ref[block * LANES:(block + 1) * LANES, columns_at] * spread
                )
            at += 1


def normed(columns, powers, blocks):
    rows = sum(block.shape[0] for block in blocks)
    width = blocks[0].shape[1]
    return pl.pallas_call(
        functools.partial(norm_kernel, columns, len(powers)),
        in_specs=[vmem()] * (len(powers) + len(blocks)),
        out_specs=vmem(),
        out_shape=jax.ShapeDtypeStruct((rows, width), jnp.float32),
        cost_estimate=cost(rows * width, 8 * rows * width),
        compiler_params=params(8),
    )(*powers, *blocks)


def square_lanes(first_factor, second_factor, result_in, pivot_scale):
    return square_lanes_body(first_factor, second_factor, result_in, pivot_scale)


def square_lanes_body(first_factor, second_factor, result_in, pivot_scale):
    bands, lanes = lax.axis_size("band"), lax.axis_size("lane")
    chips = bands // CORES
    band, lane = lax.axis_index("band"), lax.axis_index("lane")
    z, core = band // CORES, band % CORES
    agree = jnp.where(z % 2 == lane % 2, 1, 0)
    where = jnp.stack([z, core, lane, agree]).astype(jnp.int32)

    def send(axis, perm, value):
        return lax.ppermute(value, axis, perm)

    def across(distance):
        return [(l, l ^ distance) for l in range(lanes)]

    def some(target, wanted):
        pairs = []
        for b in range(bands):
            for l in range(lanes):
                if ((b // CORES) % 2 == l % 2) == wanted:
                    to_b, to_l = target(b, l)
                    pairs.append((b * lanes + l, to_b * lanes + to_l))
        return pairs

    both = ("band", "lane")
    swap = [(b, b ^ 1) for b in range(bands)]

    def px(value):
        return send("lane", across(1), value)

    def py(value):
        return send("lane", across(2), value)

    def swapped(value):
        return value, send("band", swap, value)

    def to_plane(distance):
        return lambda b, l: (b ^ (CORES * distance), l)

    def to_side(distance):
        return lambda b, l: (b ^ (CORES * distance), l ^ 1)

    r0 = second_factor
    side = [swapped(send(both, some(to_side(at), False), r0)) for at in range(chips)]
    line = [(r0, None)] + [
        swapped(send(both, some(to_plane(at), True), r0))
        for at in range(1, chips)
    ]
    at_hand = (swapped(r0), line[1])
    later = (line[2], line[3])
    far = [(0, side[0]), (2, side[2]), (1, side[1]), (3, side[3])]

    lane_at = where[2:3]
    owns = [
        *scaled_pieces(lane_at, first_factor, pivot_scale, 0, 2, 2),
        *scaled_pieces(lane_at, first_factor, pivot_scale, 1, 2, 2),
    ]
    sides = [py(own) for own in owns]

    sent0, far_right = partial_first(where, far, owns[0], sides[0])
    sents = [sent0]
    for own, side in zip(owns[1:], sides[1:]):
        sents += partials(far_right, [own], [side])
    backs = [px(sent) for sent in sents]

    keeps = kept(where, (0, 1), at_hand, result_in, owns, sides)
    n = len(owns) - 1
    outs, power, late_right = joined(
        where, (2, 3), later, keeps[:n], backs[:n], owns[:n], sides[:n], ()
    )
    last_outs, power, _ = joined(
        where, (2, 3), later, keeps[n:], backs[n:], owns[n:], sides[n:], (late_right, power)
    )
    outs = [*outs, *last_outs]
    columns = result_in.shape[1] * lanes
    powers = [power, px(power), py(power), send("lane", across(3), power)]
    return normed(columns, powers, outs)


def any_lanes(first_factor, second_factor, result_in, pivot_scale):
    share = first_factor.shape[1]
    part_scale = lax.dynamic_slice_in_dim(pivot_scale, lax.axis_index("lane") * share, share)
    scaled_left = (first_factor.astype(jnp.float32) * part_scale).astype(jnp.bfloat16)
    left_line = lax.all_gather(scaled_left, "lane", axis=1, tiled=True)
    right_line = lax.all_gather(second_factor, "band", axis=0, tiled=True)
    total = jnp.dot(left_line, right_line, preferred_element_type=jnp.float32)
    updated = result_in - total
    row_power = lax.psum(jnp.sum(updated * updated, axis=1), "lane")
    columns = updated.shape[1] * lax.axis_size("lane")
    return updated * lax.rsqrt(row_power / columns + EPS)[:, None]


def solution(mesh):
    square = mesh.shape["lane"] == 4 and mesh.shape["band"] == 4 * CORES
    return jax.shard_map(
        square_lanes if square else any_lanes,
        mesh=mesh,
        in_specs=(P("band", "lane"), P("band", "lane"), P("band", "lane"), P()),
        out_specs=P("band", "lane"),
        check_vma=False,
    )
```

```python
import functools

import jax
import jax.numpy as jnp
from jax import lax
from jax.experimental import pallas as pl
from jax.experimental.pallas import tpu as pltpu
from jax.sharding import PartitionSpec as P


CORES = 2
EPS = 1e-06
LANES = 128
MIB = 1024 * 1024


def cost(flops, nbytes):
    return pl.CostEstimate(flops=int(flops), bytes_accessed=int(nbytes), transcendentals=0)


def vmem():
    return pl.BlockSpec(memory_space=pltpu.VMEM)


def params(mib):
    return pltpu.CompilerParams(vmem_limit_bytes=mib * MIB)


def smem():
    return pl.BlockSpec(memory_space=pltpu.SMEM)


def scale_kernel(lane_ref, left_ref, scale_ref, *outs):
    scale = scale_ref[...].reshape(1, -1)
    height = outs[0].shape[0]
    for at, out in enumerate(outs):
        rows = left_ref[at * height:(at + 1) * height, :]
        out[...] = (rows.astype(jnp.float32) * scale).astype(jnp.bfloat16)


def scaled_pieces(lane, left, scale, block, blocks, count):
    rows, depth = left.shape
    height = rows // blocks
    piece = jax.ShapeDtypeStruct((height // count, depth), jnp.bfloat16)
    return pl.pallas_call(
        scale_kernel,
        grid_spec=pltpu.PrefetchScalarGridSpec(
            num_scalar_prefetch=1,
            grid=(1,),
            in_specs=[
                pl.BlockSpec((height, depth), lambda i, lane: (block, 0)),
                pl.BlockSpec((depth,), lambda i, lane: (lane[0],)),
            ],
            out_specs=[pl.BlockSpec(piece.shape, lambda i, lane: (0, 0))] * count,
        ),
        out_shape=[piece] * count,
        cost_estimate=cost(2 * height * depth, 4 * height * depth),
        compiler_params=params(8),
    )(lane, left, scale)


def bring_one(where_ref, agreeing, others, out, sems):
    core, agree = where_ref[1], where_ref[3]

    def one(pair):
        copies = []
        for part, (source, half) in enumerate(((pair[0], core), (pair[1], 1 - core))):
            depth = source.shape[0]
            start = pl.multiple_of(half * depth, depth)
            copies.append(
                pltpu.make_async_copy(source, out.at[pl.ds(start, depth), :], sems.at[part])
            )
        for copy in copies:
            copy.start()
        for copy in copies:
            copy.wait()

    @pl.when(agree == 1)
    def _():
        one(agreeing)

    @pl.when(agree == 0)
    def _():
        one(others)


def is_own(where_ref, distances):
    z, lane, agree = where_ref[0], where_ref[2], where_ref[3]
    distance = jnp.where(agree == 1, distances[0], distances[1])
    return lax.bitwise_xor(z, distance) == lane


def dot(left, right):
    return jnp.dot(left, right, preferred_element_type=jnp.float32)


def pick(own, do, own_refs, side_refs):
    pl.when(own)(lambda: do(own_refs))
    pl.when(jnp.logical_not(own))(lambda: do(side_refs))


def partial_early(where, distances, pieces, own, side):
    rows, deep = own.shape
    width = pieces[0][0].shape[1]

    def kernel(where_ref, *refs):
        own_ref, side_ref, part_ref, right_ref, sems = refs[4:]
        bring_one(where_ref, refs[:2], refs[2:4], right_ref, sems)

        def product(left):
            part_ref[...] = dot(left[...], right_ref[...])

        pick(is_own(where_ref, distances), product, own_ref, side_ref)

    return pl.pallas_call(
        kernel,
        in_specs=[smem()] + [pl.BlockSpec(memory_space=pl.ANY)] * 4 + [vmem()] * 2,
        out_specs=[vmem()] * 2,
        out_shape=[
            jax.ShapeDtypeStruct((rows, width), jnp.float32),
            jax.ShapeDtypeStruct((deep, width), jnp.bfloat16),
        ],
        scratch_shapes=[pltpu.SemaphoreType.DMA((CORES,))],
        cost_estimate=cost(2 * rows * deep * width, 4 * deep * width),
        compiler_params=params(12),
    )(where, *pieces[0], *pieces[1], own, side)


def partial_late(where, distances, pieces, part, own, side):
    rows, deep = own.shape
    width = part.shape[1]

    def kernel(where_ref, *refs):
        part_ref, own_ref, side_ref, sent_ref, right_ref, sems = refs[4:]
        bring_one(where_ref, refs[:2], refs[2:4], right_ref, sems)

        def product(left):
            sent_ref[...] = (part_ref[...] + dot(left[...], right_ref[...])).astype(jnp.bfloat16)

        pick(is_own(where_ref, distances), product, own_ref, side_ref)

    return pl.pallas_call(
        kernel,
        in_specs=[smem()] + [pl.BlockSpec(memory_space=pl.ANY)] * 4 + [vmem()] * 3,
        out_specs=[vmem()] * 2,
        out_shape=[
            jax.ShapeDtypeStruct((rows, width), jnp.bfloat16),
            jax.ShapeDtypeStruct((deep, width), jnp.bfloat16),
        ],
        scratch_shapes=[pltpu.SemaphoreType.DMA((CORES,))],
        cost_estimate=cost(2 * rows * deep * width, 4 * deep * width),
        compiler_params=params(12),
    )(where, *pieces[0], *pieces[1], part, own, side)


def partials(where, distances, early, late, own, side):
    rows, deep = own.shape
    width = early.shape[1]

    def kernel(where_ref, early_ref, late_ref, own_ref, side_ref, out):
        def products(lefts):
            total = dot(lefts[0][...], early_ref[...]) + dot(lefts[1][...], late_ref[...])
            out[...] = total.astype(jnp.bfloat16)

        pick(is_own(where_ref, distances), products, (own_ref, side_ref), (side_ref, own_ref))

    return pl.pallas_call(
        kernel,
        in_specs=[smem()] + [vmem()] * 4,
        out_specs=vmem(),
        out_shape=jax.ShapeDtypeStruct((rows, width), jnp.bfloat16),
        cost_estimate=cost(4 * rows * deep * width, 4 * deep * width),
        compiler_params=params(16),
    )(where, early, late, own, side)


def kept(where, distances, pieces, base, first, owns, sides):
    count = len(owns)
    height, deep = owns[0].shape
    width = base.shape[1]

    def kernel(where_ref, *refs):
        base_ref, lefts = refs[4], refs[5:5 + 2 * count]
        outs, right_ref, sems = refs[5 + 2 * count:5 + 3 * count], refs[-2], refs[-1]
        bring_one(where_ref, refs[:2], refs[2:4], right_ref, sems)
        own = is_own(where_ref, distances)

        def products(chosen):
            for at in range(count):
                row = (first + at) * height
                outs[at][...] = base_ref[row:row + height, :] - dot(chosen[at][...], right_ref[...])

        pl.when(own)(lambda: products(lefts[:count]))
        pl.when(jnp.logical_not(own))(lambda: products(lefts[count:]))

    flops = 2 * count * height * deep * width
    return pl.pallas_call(
        kernel,
        in_specs=[smem()] + [pl.BlockSpec(memory_space=pl.ANY)] * 4 + [vmem()] * (1 + 2 * count),
        out_specs=[vmem()] * count,
        out_shape=[jax.ShapeDtypeStruct((height, width), jnp.float32)] * count,
        scratch_shapes=[
            pltpu.VMEM((deep, width), jnp.bfloat16), pltpu.SemaphoreType.DMA((CORES,))
        ],
        cost_estimate=cost(flops, flops / 512),
        compiler_params=params(24),
    )(where, *pieces[0], *pieces[1], base, *owns, *sides)


def power_rows(block):
    squares = block * block
    folded = squares[:, :LANES]
    for at in range(1, block.shape[1] // LANES):
        folded = folded + squares[:, at * LANES:(at + 1) * LANES]
    return jnp.sum(folded.T, axis=0, keepdims=True)


def put_powers(ref, power_ref, at):
    for block in range(ref.shape[0] // LANES):
        power_ref[at:at + 1, :] = power_rows(ref[block * LANES:(block + 1) * LANES, :])
        at += 1
    return at


def joined(where, distances, pieces, keeps, gots, owns, sides, before):
    count = len(keeps)
    height, deep = owns[0].shape
    width = keeps[0].shape[1]
    block = jax.ShapeDtypeStruct((deep, width), jnp.bfloat16)
    done = before[1].shape[0] if before else 0
    n_first = 2 if before else 4

    def kernel(where_ref, *refs):
        first, rest = refs[:n_first], refs[n_first:]
        kept_refs, got_refs, lefts = rest[:count], rest[count:2 * count], rest[2 * count:4 * count]
        outs, power_ref = rest[4 * count:5 * count], rest[5 * count]
        if before:
            right_ref = first[0]
            power_ref[:done, :] = first[1][...]
        else:
            right_ref = rest[5 * count + 1]
            bring_one(where_ref, first[:2], first[2:], right_ref, rest[5 * count + 2])
        own = is_own(where_ref, distances)

        def products(chosen):
            for at in range(count):
                total = dot(chosen[at][...], right_ref[...])
                outs[at][...] = kept_refs[at][...] - total - got_refs[at][...].astype(jnp.float32)

        pl.when(own)(lambda: products(lefts[:count]))
        pl.when(jnp.logical_not(own))(lambda: products(lefts[count:]))
        at = done
        for out in outs:
            at = put_powers(out, power_ref, at)

    flops = 2 * count * height * deep * width
    results = pl.pallas_call(
        kernel,
        in_specs=[smem()]
        + [vmem() if before else pl.BlockSpec(memory_space=pl.ANY)] * n_first
        + [vmem()] * (4 * count),
        out_specs=[vmem()] * (count + 1 + (not before)),
        out_shape=[jax.ShapeDtypeStruct((height, width), jnp.float32)] * count
        + [jax.ShapeDtypeStruct((done + count * height // LANES, LANES), jnp.float32)]
        + ([] if before else [block]),
        scratch_shapes=[] if before else [pltpu.SemaphoreType.DMA((CORES,))],
        cost_estimate=cost(flops, flops / 256),
        compiler_params=params(16),
    )(where, *(before if before else (*pieces[0], *pieces[1])), *keeps, *gots, *owns, *sides)
    return results[:count], results[count], None if before else results[count + 1]


def norm_kernel(columns, n_power, *refs):
    powers, blocks, out = refs[:n_power], refs[n_power:-1], refs[-1]
    power = powers[0][...]
    for ref in powers[1:]:
        power = power + ref[...]
    factor = lax.rsqrt(power / columns + EPS)
    at = 0
    for ref in blocks:
        for block in range(ref.shape[0] // LANES):
            spread = jnp.broadcast_to(factor[at:at + 1, :], (LANES, LANES)).T
            for tile in range(ref.shape[1] // LANES):
                columns_at = slice(tile * LANES, (tile + 1) * LANES)
                out[at * LANES:(at + 1) * LANES, columns_at] = (
                    ref[block * LANES:(block + 1) * LANES, columns_at] * spread
                )
            at += 1


def normed(columns, powers, blocks):
    rows = sum(block.shape[0] for block in blocks)
    width = blocks[0].shape[1]
    return pl.pallas_call(
        functools.partial(norm_kernel, columns, len(powers)),
        in_specs=[vmem()] * (len(powers) + len(blocks)),
        out_specs=vmem(),
        out_shape=jax.ShapeDtypeStruct((rows, width), jnp.float32),
        cost_estimate=cost(rows * width, 8 * rows * width),
        compiler_params=params(8),
    )(*powers, *blocks)


def square_lanes(first_factor, second_factor, result_in, pivot_scale):
    return square_lanes_body(first_factor, second_factor, result_in, pivot_scale)


def square_lanes_body(first_factor, second_factor, result_in, pivot_scale):
    bands, lanes = lax.axis_size("band"), lax.axis_size("lane")
    band, lane = lax.axis_index("band"), lax.axis_index("lane")
    z, core = band // CORES, band % CORES
    agree = jnp.where(z % 2 == lane % 2, 1, 0)
    where = jnp.stack([z, core, lane, agree]).astype(jnp.int32)

    def send(axis, perm, value):
        return lax.ppermute(value, axis, perm)

    def across(distance):
        return [(l, l ^ distance) for l in range(lanes)]

    def some(target, wanted):
        pairs = []
        for b in range(bands):
            for l in range(lanes):
                if ((b // CORES) % 2 == l % 2) == wanted:
                    to_b, to_l = target(b, l)
                    pairs.append((b * lanes + l, to_b * lanes + to_l))
        return pairs

    both = ("band", "lane")
    swap = [(b, b ^ 1) for b in range(bands)]

    def px(value):
        return send("lane", across(1), value)

    def py(value):
        return send("lane", across(2), value)

    def swapped(value):
        return value, send("band", swap, value)

    def to_plane(distance):
        return lambda b, l: (b ^ (CORES * distance), l)

    def to_side(distance):
        return lambda b, l: (b ^ (CORES * distance), l ^ 1)

    r0 = second_factor

    def sent(*pairs):
        return swapped(send(both, [pair for some in pairs for pair in some], r0))

    d0 = sent(some(to_side(0), False))
    m1 = sent(some(to_side(1), False), some(to_plane(2), True))
    m2 = sent(some(to_side(2), False), some(to_plane(1), True))
    d3 = sent(some(to_side(3), False))
    k3 = sent(some(to_plane(3), True))
    side, line = [d0, m1, m2, d3], [None, m2, m1, k3]
    at_hand = (swapped(r0), line[1])
    later = (line[2], line[3])

    lane_at = where[2:3]
    owns = [
        *scaled_pieces(lane_at, first_factor, pivot_scale, 0, 2, 2),
        *scaled_pieces(lane_at, first_factor, pivot_scale, 1, 2, 2),
    ]
    sides = [py(own) for own in owns]

    soon, then = (0, 3), (2, 1)
    part, early = partial_early(where, soon, [side[at] for at in soon], owns[0], sides[0])
    sent0, late = partial_late(where, then, [side[at] for at in then], part, owns[0], sides[0])
    sents = [sent0] + [
        partials(where, soon, early, late, own, y) for own, y in zip(owns[1:], sides[1:])
    ]
    backs = [px(sent) for sent in sents]

    n = len(owns) - 1
    keeps = kept(where, (0, 1), at_hand, result_in, 0, owns[:n], sides[:n])
    keeps = [*keeps, *kept(where, (0, 1), at_hand, result_in, n, owns[n:], sides[n:])]
    outs, power, late_right = joined(
        where, (2, 3), later, keeps[:n], backs[:n], owns[:n], sides[:n], ()
    )
    last_outs, power, _ = joined(
        where, (2, 3), later, keeps[n:], backs[n:], owns[n:], sides[n:], (late_right, power)
    )
    outs = [*outs, *last_outs]
    columns = result_in.shape[1] * lanes
    powers = [power, px(power), py(power), send("lane", across(3), power)]
    return normed(columns, powers, outs)


def any_lanes(first_factor, second_factor, result_in, pivot_scale):
    share = first_factor.shape[1]
    part_scale = lax.dynamic_slice_in_dim(pivot_scale, lax.axis_index("lane") * share, share)
    scaled_left = (first_factor.astype(jnp.float32) * part_scale).astype(jnp.bfloat16)
    left_line = lax.all_gather(scaled_left, "lane", axis=1, tiled=True)
    right_line = lax.all_gather(second_factor, "band", axis=0, tiled=True)
    total = jnp.dot(left_line, right_line, preferred_element_type=jnp.float32)
    updated = result_in - total
    row_power = lax.psum(jnp.sum(updated * updated, axis=1), "lane")
    columns = updated.shape[1] * lax.axis_size("lane")
    return updated * lax.rsqrt(row_power / columns + EPS)[:, None]


def solution(mesh):
    square = mesh.shape["lane"] == 4 and mesh.shape["band"] == 4 * CORES
    return jax.shard_map(
        square_lanes if square else any_lanes,
        mesh=mesh,
        in_specs=(P("band", "lane"), P("band", "lane"), P("band", "lane"), P()),
        out_specs=P("band", "lane"),
        check_vma=False,
    )
```
